16 devices in a mesh: dp: 1, sp: 16 (over x, y, z, core).
Axes of the slice: x: 2, y: 2, z: 2, core: 2. Of those that a mesh axis runs over, the one named last changes fastest.
Arguments:
- x: bfloat16 [2048, 14336], P(('dp', 'sp'))
- gain: bfloat16 [14336], replicated
- wq: bfloat16 [14336, 14336], replicated
- wk: bfloat16 [14336, 14336], replicated
- wv: bfloat16 [14336, 14336], replicated
- wo: bfloat16 [14336, 14336], replicated
Outputs:
- output: bfloat16 [2048, 14336], P(('dp', 'sp'))
All inputs are finite; a program needn't handle non-finite values.
Results may differ from the reference program's by a relative error of at most 0.012.
Values are sent between devices in bfloat16 or wider.
A program may use at most 3.75 GiB of HBM per device.

```python
import jax
import jax.numpy as jnp
from jax import lax

ROWS = 2048
D = 14336
HEADS = 112
KV_HEADS = 112
HEAD = 128
THETA = 10000


def setup_inputs(seed: int = 0, part: int = 0) -> dict:
    kx, kn, kq, kk, kv, ko = jax.random.split(jax.random.key(seed), 6)

    def weights(key, rows, columns):
        return jax.random.normal(key, (rows, columns), jnp.float32) * rows**-0.5

    drawn = {
        "x": jax.random.normal(jax.random.fold_in(kx, part), (ROWS, D), jnp.float32),
        "gain": 1 + 0.1 * jax.random.normal(kn, (D,), jnp.float32),
        "wq": 2 * weights(kq, D, HEADS * HEAD),
        "wk": 2 * weights(kk, D, KV_HEADS * HEAD),
        "wv": 4 * weights(kv, D, KV_HEADS * HEAD),
        "wo": weights(ko, HEADS * HEAD, D),
    }
    return {k: v.astype(jnp.bfloat16) for k, v in drawn.items()}


def normed(x, gain):
    wide = x.astype(jnp.float32)
    scale = lax.rsqrt(jnp.mean(wide * wide, -1, keepdims=True) + 1e-6)
    return (wide * scale * gain.astype(jnp.float32)).astype(jnp.bfloat16)


def turned(t, place, theta):
    half = t.shape[-1] // 2
    angle = place.astype(jnp.float32)[:, None] * theta ** (-jnp.arange(half, dtype=jnp.float32) / half)
    cos, sin = jnp.cos(angle)[:, None], jnp.sin(angle)[:, None]
    a, b = t[..., :half].astype(jnp.float32), t[..., half:].astype(jnp.float32)
    return jnp.concatenate([a * cos - b * sin, b * cos + a * sin], -1).astype(jnp.bfloat16)


def matmul(a, w):
    return jnp.dot(a, w, preferred_element_type=jnp.float32).astype(jnp.bfloat16)


def einsum(form, a, b):
    return jnp.einsum(form, a.astype(jnp.float32), b.astype(jnp.float32))


def attention(q, k, v):
    scores = einsum("tgsd,ugd->gstu", q, k) * q.shape[-1] ** -0.5
    token = jnp.arange(q.shape[0])
    scores = jnp.where(token[:, None] >= token, scores, -jnp.inf)
    weights = jax.nn.softmax(scores, -1).astype(jnp.bfloat16)
    return einsum("gstu,ugd->tgsd", weights, v).astype(jnp.bfloat16)


def reference(x, gain, wq, wk, wv, wo):
    a, place = normed(x, gain), jnp.arange(ROWS)
    q = turned(matmul(a, wq).reshape(ROWS, HEADS, HEAD), place, THETA).reshape(ROWS, KV_HEADS, -1, HEAD)
    k = turned(matmul(a, wk).reshape(ROWS, KV_HEADS, HEAD), place, THETA)
    v = matmul(a, wv).reshape(ROWS, KV_HEADS, HEAD)
    seen = attention(q, k, v).reshape(ROWS, HEADS * HEAD)
    return (x.astype(jnp.float32) + jnp.dot(seen, wo, preferred_element_type=jnp.float32)).astype(jnp.bfloat16)
```

```python
import functools

import jax
import jax.numpy as jnp
from jax import lax
from jax.experimental import pallas as pl
from jax.experimental.pallas import tpu as pltpu
from jax.sharding import PartitionSpec as P

HEAD = 128
THETA = 10000
NEG = -1e30
LOG2E = 1.4426950408889634

D = 14336
OWN = 128
PAIR = 256
CHIPS = 8
STEPS = 7
CUT = 2048
CUTS = D // CUT
WIDE = CHIPS * HEAD
SLOTS = 5
LAG = 3
TURNS = 3
TOKENS = CHIPS * PAIR
BLOCK = 512
TOTAL = STEPS * CUTS * 4


def _dot(a, b, ca, cb):
    return lax.dot_general(a, b, (((ca,), (cb,)), ((), ())), preferred_element_type=jnp.float32)


def _kernel(a_hbm, x_hbm, cos_ref, sin_ref, wq, wk, wv, wo, y_hbm, a_buf, ring, acc, yacc, ypeer, sbuf, rbuf, obuf, seen, top_s, mix_s,
            ring_sem, a_loc, a_send, a_recv, q_send, q_recv, o_send, o_recv, y_send, y_recv, x_sem, out_sem):
    me = lax.axis_index("sp")
    core, chip = lax.rem(me, 2), lax.div(me, 2)
    partner = me + 1 - 2 * core
    mine = pl.ds(pl.multiple_of(core * OWN, OWN), OWN)
    other = pl.ds(pl.multiple_of((1 - core) * OWN, OWN), OWN)
    peers = [lax.rem(chip + n, CHIPS) for n in range(1, CHIPS)]

    def remote(src, dst, send, recv, device):
        return pltpu.make_async_remote_copy(src_ref=src, dst_ref=dst, send_sem=send, recv_sem=recv, device_id={"sp": device},
                                            device_id_type=pl.DeviceIdType.MESH)

    def start(t):
        early, late = t < 3 * 21, t >= 3 * 21 + 4 * 28
        stage = jnp.where(early, lax.div(t, 21), jnp.where(late, 7 + lax.div(t - 175, 7), 3 + lax.div(t - 63, 28)))
        unit = jnp.where(early, 7 + lax.rem(t, 21), jnp.where(late, lax.rem(t - 175, 7), lax.rem(t - 63, 28)))
        slot = lax.rem(t, SLOTS)
        for i, w in enumerate((wo, wq, wk, wv)):

            @pl.when((unit >= 7 * i) & (unit < 7 * i + 7) & (t < TOTAL))
            def _():
                n = unit - 7 * i
                for h in range(2):
                    if i == 0:
                        rows, columns = (core * STEPS + stage - LAG) * WIDE, n * CUT + h * WIDE
                    else:
                        rows, columns = n * CUT + h * WIDE, (core * STEPS + stage) * WIDE
                    part = w.at[pl.ds(pl.multiple_of(rows, WIDE), WIDE), pl.ds(pl.multiple_of(columns, WIDE), WIDE)]
                    pltpu.make_async_copy(part, ring.at[slot, h], ring_sem.at[slot, h]).start()

    def arrive(t):
        slot = lax.rem(t, SLOTS)
        for h in range(2):
            pltpu.make_async_copy(wq.at[pl.ds(0, WIDE), pl.ds(0, WIDE)], ring.at[slot, h], ring_sem.at[slot, h]).wait()
        start(t + SLOTS - 1)
        return slot

    for t in range(SLOTS - 1):
        start(jnp.int32(t))
    for n in range(CUTS):
        pltpu.make_async_copy(a_hbm.at[:, pl.ds(n * CUT, CUT)], a_buf.at[n, mine, :], a_loc.at[n]).start()

    barrier = pltpu.get_barrier_semaphore()
    pl.semaphore_signal(barrier, inc=1, device_id={"sp": partner}, device_id_type=pl.DeviceIdType.MESH)
    for p in peers:
        pl.semaphore_signal(barrier, inc=1, device_id={"sp": 2 * p + core}, device_id_type=pl.DeviceIdType.MESH)
    pl.semaphore_wait(barrier, CHIPS)

    def swap(n):
        return remote(a_hbm.at[:, pl.ds(n * CUT, CUT)], a_buf.at[n, mine, :], a_send.at[n], a_recv.at[n], partner)

    def swapped(n):
        return remote(a_hbm.at[:, pl.ds(n * CUT, CUT)], a_buf.at[n, other, :], a_send.at[n], a_recv.at[n], partner)

    for n in range(CUTS):
        swap(n).start()
    for n in range(CUTS):
        pltpu.make_async_copy(a_hbm.at[:, pl.ds(n * CUT, CUT)], a_buf.at[n, mine, :], a_loc.at[n]).wait()
        swapped(n).wait()

    def sends(i, turn):
        for n, p in enumerate(peers):
            yield remote(sbuf.at[i, p], rbuf.at[turn, i, chip], q_send.at[i, n], q_recv.at[turn, i, chip], 2 * p + core)

    def ship(i, turn):
        for copy in sends(i, turn):
            copy.start()
        rbuf[turn, i, chip] = sbuf[i, chip]

    def projections(stage, first):
        turn = lax.rem(stage, TURNS)
        for i in range(3):

            def chunk(n, fresh):
                slot = arrive(first + 7 * i + n)
                got = _dot(a_buf[n], ring[slot].reshape(CUT, WIDE), 1, 0)
                if fresh:
                    acc[...] = got
                else:
                    acc[...] += got

            chunk(0, True)
            if i:
                ship(i - 1, turn)

            def more(n, _):
                chunk(n, False)

            lax.fori_loop(1, CUTS, more, None)

            @pl.when(stage > 0)
            def _():
                for copy in sends(i, turn):
                    copy.wait_send()

            for h in range(CHIPS):
                t = acc[:, h * HEAD : (h + 1) * HEAD].astype(jnp.bfloat16)
                if i < 2:
                    t = t.astype(jnp.float32)
                    t = (t * cos_ref[...] + pltpu.roll(t, HEAD // 2, 1) * sin_ref[...]).astype(jnp.bfloat16)
                sbuf[i, h] = t

    def attend(turn):
        e = HEAD**-0.5 * LOG2E
        blocks = TOKENS // BLOCK
        per = BLOCK // PAIR
        ones = jnp.ones((8, BLOCK), jnp.bfloat16)
        visible = lax.broadcasted_iota(jnp.int32, (BLOCK, BLOCK), 1) >= lax.broadcasted_iota(jnp.int32, (BLOCK, BLOCK), 0)
        part = lambda i, j: rbuf[turn, i, j * per : (j + 1) * per].reshape(BLOCK, HEAD)
        for j in range(blocks):
            keys = part(1, j)
            values = jnp.concatenate([part(2, j).T, ones], axis=0)
            scores = [_dot(keys, part(0, i), 1, 1) for i in range(j, blocks)]
            weights, keeps = [], []
            for i, s in zip(range(j, blocks), scores):
                if i == j:
                    s = jnp.where(visible, s, 2 * NEG)
                top = s.max(axis=0, keepdims=True)
                if j:
                    old = top_s[i : i + 1, :]
                    top = jnp.maximum(old, top)
                    keeps.append(jnp.exp2((old - top) * e))
                else:
                    keeps.append(None)
                top_s[i : i + 1, :] = top
                weights.append(jnp.exp2((s - top) * e).astype(jnp.bfloat16))
            for i, p, keep in zip(range(j, blocks), weights, keeps):
                new = _dot(values, p, 1, 0)
                if j:
                    new = mix_s[i] * keep + new
                if i == j:
                    done = (new[:HEAD] * (1 / new[HEAD : HEAD + 1])).T.astype(jnp.bfloat16)
                    obuf[i * per : (i + 1) * per] = done.reshape(per, PAIR, HEAD)
                else:
                    mix_s[i] = new

    def outs(turn):
        for n, p in enumerate(peers):
            yield remote(obuf.at[p], seen.at[turn, chip], o_send.at[n], o_recv.at[turn, chip], 2 * p + core)

    def halves(n):
        return remote(yacc.at[n, other, :], ypeer.at[n], y_send.at[n], y_recv.at[n], partner)

    def stages(stage, _):
        first = 21 * jnp.minimum(stage, 7) + 7 * jnp.maximum(stage - 3, 0)

        @pl.when(stage >= LAG)
        def _():
            turn = lax.rem(stage - LAG, TURNS)
            for p in peers:
                remote(obuf.at[p], seen.at[turn, p], o_send.at[0], o_recv.at[turn, p], 2 * p + core).wait_recv()

            def chunk(n, fresh):
                slot = arrive(first + n)
                lhs = jnp.concatenate([seen[turn, h] for h in range(CHIPS)], axis=1)
                for h in range(2):
                    here = slice(h * WIDE, (h + 1) * WIDE)
                    got = _dot(lhs, ring[slot, h], 1, 0)
                    if fresh:
                        yacc[n, :, here] = got
                    else:
                        yacc[n, :, here] += got

            @pl.when(stage == LAG)
            def _():
                lax.fori_loop(0, CUTS, lambda n, _: chunk(n, True), None)

            @pl.when(stage > LAG)
            def _():
                def more(n, _):
                    chunk(n, False)

                    @pl.when((stage == STEPS + LAG - 1) & (n > 0))
                    def _():
                        halves(n - 1).start()

                lax.fori_loop(0, CUTS, more, None)

        @pl.when(stage < STEPS)
        def _():
            projections(stage, first + 7 * jnp.minimum(jnp.maximum(stage - 2, 0), 1))

        @pl.when((stage >= 1) & (stage <= STEPS))
        def _():
            turn = lax.rem(stage - 1, TURNS)
            for i in range(3):
                for p in peers:
                    remote(sbuf.at[i, p], rbuf.at[turn, i, p], q_send.at[i, 0], q_recv.at[turn, i, p], 2 * p + core).wait_recv()

        @pl.when(stage < STEPS)
        def _():
            ship(2, lax.rem(stage, TURNS))

        @pl.when((stage >= 1) & (stage <= STEPS))
        def _():
            turn = lax.rem(stage - 1, TURNS)

            @pl.when(stage > 1)
            def _():
                for copy in outs(turn):
                    copy.wait_send()

            attend(turn)
            for copy in outs(turn):
                copy.start()
            seen[turn, chip] = obuf[chip]

        @pl.when(stage == STEPS)
        def _():
            for n in range(CUTS):
                pltpu.make_async_copy(x_hbm.at[:, pl.ds(n * CUT, CUT)], a_buf.at[n, pl.ds(0, OWN), :], x_sem.at[n]).start()

    lax.fori_loop(0, STEPS + LAG, stages, None)
    halves(CUTS - 1).start()
    for i in range(3):
        for copy in sends(i, 0):
            copy.wait_send()
    for copy in outs(0):
        copy.wait_send()

    def result(n):
        return pltpu.make_async_copy(a_buf.at[n, pl.ds(OWN, OWN), :], y_hbm.at[:, pl.ds(n * CUT, CUT)], out_sem.at[n])

    for n in range(CUTS):
        pltpu.make_async_copy(x_hbm.at[:, pl.ds(n * CUT, CUT)], a_buf.at[n, pl.ds(0, OWN), :], x_sem.at[n]).wait()
        halves(n).wait_recv()
        total = yacc[n, mine, :] + ypeer[n]
        a_buf[n, OWN:, :] = (a_buf[n, :OWN, :].astype(jnp.float32) + total).astype(jnp.bfloat16)
        if n:
            result(n - 1).start()
    result(CUTS - 1).start()
    for n in range(CUTS):
        halves(n).wait_send()
        result(n).wait()


def normed(x, gain):
    wide = x.astype(jnp.float32)
    scale = lax.rsqrt(jnp.mean(wide * wide, -1, keepdims=True) + 1e-6)
    return (wide * scale * gain.astype(jnp.float32)).astype(jnp.bfloat16)


def layer(a, x, cos, sin, wq, wk, wv, wo):
    dma = pltpu.SemaphoreType.DMA
    anywhere, vmem = pl.BlockSpec(memory_space=pl.ANY), pl.BlockSpec(memory_space=pltpu.VMEM)
    return pl.pallas_call(
        _kernel,
        out_shape=jax.ShapeDtypeStruct((OWN, D), jnp.bfloat16),
        in_specs=[anywhere, anywhere, vmem, vmem] + [anywhere] * 4,
        out_specs=anywhere,
        scratch_shapes=[
            pltpu.VMEM((CUTS, PAIR, CUT), jnp.bfloat16),
            pltpu.VMEM((SLOTS, 2, WIDE, WIDE), jnp.bfloat16),
            pltpu.VMEM((PAIR, WIDE), jnp.float32),
            pltpu.VMEM((CUTS, PAIR, CUT), jnp.float32),
            pltpu.VMEM((CUTS, OWN, CUT), jnp.float32),
            pltpu.VMEM((3, CHIPS, PAIR, HEAD), jnp.bfloat16),
            pltpu.VMEM((TURNS, 3, CHIPS, PAIR, HEAD), jnp.bfloat16),
            pltpu.VMEM((CHIPS, PAIR, HEAD), jnp.bfloat16),
            pltpu.VMEM((TURNS, CHIPS, PAIR, HEAD), jnp.bfloat16),
            pltpu.VMEM((TOKENS // BLOCK, BLOCK), jnp.float32),
            pltpu.VMEM((TOKENS // BLOCK, HEAD + 8, BLOCK), jnp.float32),
            dma((SLOTS, 2)),
            dma((CUTS,)),
            dma((CUTS,)),
            dma((CUTS,)),
            dma((3, CHIPS - 1)),
            dma((TURNS, 3, CHIPS)),
            dma((CHIPS - 1,)),
            dma((TURNS, CHIPS)),
            dma((CUTS,)),
            dma((CUTS,)),
            dma((CUTS,)),
            dma((CUTS,)),
        ],
        compiler_params=pltpu.CompilerParams(collective_id=0, has_side_effects=True, vmem_limit_bytes=67043328),
        cost_estimate=pl.CostEstimate(flops=8 * OWN * D * D, transcendentals=STEPS * TOKENS * TOKENS, bytes_accessed=4 * D * D),
    )(a, x, cos, sin, wq, wk, wv, wo)


def solution(mesh):
    def step(x, gain, wq, wk, wv, wo):
        place = lax.div(lax.axis_index("sp"), 2) * PAIR + jnp.arange(PAIR)
        half = HEAD // 2
        angle = place.astype(jnp.float32)[:, None] * THETA ** (-jnp.arange(half, dtype=jnp.float32) / half)
        cos, sin = jnp.cos(angle), jnp.sin(angle)
        return layer(normed(x, gain), x, jnp.concatenate([cos, cos], -1), jnp.concatenate([-sin, sin], -1), wq, wk, wv, wo)

    tokens, whole = P(("dp", "sp"), None), P(None, None)
    return jax.shard_map(
        step,
        mesh=mesh,
        in_specs=(tokens, P(None), whole, whole, whole, whole),
        out_specs=tokens,
        check_vma=False,
    )
```

```python
import functools

import jax
import jax.numpy as jnp
from jax import lax
from jax.experimental import pallas as pl
from jax.experimental.pallas import tpu as pltpu
from jax.sharding import PartitionSpec as P

HEAD = 128
THETA = 10000
NEG = -1e30
LOG2E = 1.4426950408889634

D = 14336
OWN = 128
PAIR = 256
CHIPS = 8
STEPS = 7
CUT = 3584
CUTS = D // CUT
WIDE = CHIPS * HEAD
SLOTS = 3
LAG = 3
TURNS = 3
TOKENS = CHIPS * PAIR
BLOCK = 512
UNITS = 3 * CUTS
MIDDLE, LATE = LAG * UNITS, LAG * UNITS + (STEPS - LAG) * (UNITS + CUTS)
TOTAL = STEPS * CUTS * 4


def _dot(a, b, ca, cb):
    return lax.dot_general(a, b, (((ca,), (cb,)), ((), ())), preferred_element_type=jnp.float32)


def _kernel(x_hbm, gain_ref, cos_ref, sin_ref, wq, wk, wv, wo, y_hbm, a_buf, ring, acc, yacc, ypeer, sbuf, rbuf, obuf, seen, top_s, mix_s,
            ring_sem, x_in, a_send, a_recv, q_send, q_recv, o_send, o_recv, y_send, y_recv, x_sem, out_sem):
    me = lax.axis_index("sp")
    core, chip = lax.rem(me, 2), lax.div(me, 2)
    partner = me + 1 - 2 * core
    mine = pl.ds(pl.multiple_of(core * OWN, OWN), OWN)
    other = pl.ds(pl.multiple_of((1 - core) * OWN, OWN), OWN)
    peers = [lax.rem(chip + n, CHIPS) for n in range(1, CHIPS)]

    def remote(src, dst, send, recv, device):
        return pltpu.make_async_remote_copy(src_ref=src, dst_ref=dst, send_sem=send, recv_sem=recv, device_id={"sp": device},
                                            device_id_type=pl.DeviceIdType.MESH)

    def start(t):
        early, late = t < MIDDLE, t >= LATE
        stage = jnp.where(early, lax.div(t, UNITS),
                          jnp.where(late, STEPS + lax.div(t - LATE, CUTS), LAG + lax.div(t - MIDDLE, UNITS + CUTS)))
        unit = jnp.where(early, CUTS + lax.rem(t, UNITS),
                         jnp.where(late, lax.rem(t - LATE, CUTS), lax.rem(t - MIDDLE, UNITS + CUTS)))
        slot = lax.rem(t, SLOTS)

        def fetch(w, row, column, rows, columns, to_row, to_column):
            part = w.at[pl.ds(pl.multiple_of(row, 128), rows), pl.ds(pl.multiple_of(column, 128), columns)]
            to = ring.at[slot, pl.ds(to_row, rows), pl.ds(to_column, columns)]
            pltpu.make_async_copy(part, to, ring_sem.at[slot]).start()

        for i, w in enumerate((wq, wk, wv)):

            @pl.when((unit >= CUTS * (i + 1)) & (unit < CUTS * (i + 2)) & (t < TOTAL))
            def _():
                for h in range(2):
                    fetch(w, (unit - CUTS * (i + 1)) * CUT + h * (CUT // 2), (core * STEPS + stage) * WIDE, CUT // 2, WIDE, h * (CUT // 2), 0)

        @pl.when((unit < CUTS) & (t < TOTAL))
        def _():
            row, column = (core * STEPS + stage - LAG) * WIDE, unit * CUT
            for h in range(3):
                fetch(wo, row, column + h * WIDE, WIDE, WIDE, h * WIDE, 0)
            for h in range(2):
                fetch(wo, row + h * 512, column + 3 * WIDE, 512, 512, 3 * WIDE, h * 512)

    def arrive(t):
        slot = lax.rem(t, SLOTS)
        pltpu.make_async_copy(wq.at[pl.ds(0, CUT), pl.ds(0, WIDE)], ring.at[slot], ring_sem.at[slot]).wait()
        return slot

    def from_x(n, rows, sem):
        return pltpu.make_async_copy(x_hbm.at[:, pl.ds(n * CUT, CUT)], a_buf.at[n, rows, :], sem.at[n])

    barrier = pltpu.get_barrier_semaphore()
    pl.semaphore_signal(barrier, inc=1, device_id={"sp": partner}, device_id_type=pl.DeviceIdType.MESH)
    for p in peers:
        pl.semaphore_signal(barrier, inc=1, device_id={"sp": 2 * p + core}, device_id_type=pl.DeviceIdType.MESH)
    for n in range(CUTS):
        from_x(n, mine, x_in).start()
    for t in range(SLOTS):
        start(jnp.int32(t))

    def swap(n):
        return remote(a_buf.at[n, mine, :], a_buf.at[n, mine, :], a_send.at[n], a_recv.at[n], partner)

    def swapped(n):
        return remote(a_buf.at[n, other, :], a_buf.at[n, other, :], a_send.at[n], a_recv.at[n], partner)

    for n in range(CUTS):
        from_x(n, mine, x_in).wait()

    def norm(g, _):
        rows = pl.ds(pl.multiple_of(core * OWN + g * 16, 16), 16)
        wide = [a_buf[n, rows, :].astype(jnp.float32) for n in range(CUTS)]
        squares = sum(jnp.sum(w * w, axis=1, keepdims=True) for w in wide)
        scale = lax.rsqrt(squares / D + 1e-6)
        for n in range(CUTS):
            a_buf[n, rows, :] = (a_buf[n, rows, :].astype(jnp.float32) * scale * gain_ref[n]).astype(jnp.bfloat16)

    lax.fori_loop(0, OWN // 16, norm, None)
    pl.semaphore_wait(barrier, CHIPS)
    for n in range(CUTS):
        swap(n).start()
    swapped(0).wait_recv()

    def sends(i, turn):
        for n, p in enumerate(peers):
            yield remote(sbuf.at[i, p], rbuf.at[turn, i, chip], q_send.at[i, n], q_recv.at[turn, i, chip], 2 * p + core)

    def ship(i, turn):
        for copy in sends(i, turn):
            copy.start()
        rbuf[turn, i, chip] = sbuf[i, chip]

    def projections(stage, first):
        turn = lax.rem(stage, TURNS)

        def free(i):
            @pl.when(stage > 0)
            def _():
                for copy in sends(i, turn):
                    copy.wait_send()

        def finish(i):
            for h in range(CHIPS):
                t = acc[i % 2, :, h * HEAD : (h + 1) * HEAD].astype(jnp.bfloat16)
                if i < 2:
                    t = t.astype(jnp.float32)
                    t = (t * cos_ref[...] + pltpu.roll(t, HEAD // 2, 1) * sin_ref[...]).astype(jnp.bfloat16)
                sbuf[i, h] = t

        for i in range(3):

            def chunk(n, fresh):
                t = first + CUTS * i + n
                slot = arrive(t)
                if fresh and i:
                    finish(i - 1)
                got = _dot(a_buf[n], ring[slot], 1, 0)
                if fresh:
                    acc[i % 2] = got
                else:
                    acc[i % 2] += got
                start(t + SLOTS)

            if i:
                free(i - 1)
            chunk(0, True)

            def more(n, _):
                if i == 0:

                    @pl.when(stage == 0)
                    def _():
                        swapped(n).wait_recv()

                chunk(n, False)

            lax.fori_loop(1, CUTS, more, None)
            if i:
                ship(i - 1, turn)
        free(2)
        finish(2)

    def attend(turn):
        e = HEAD**-0.5 * LOG2E
        blocks = TOKENS // BLOCK
        per = BLOCK // PAIR
        ones = jnp.ones((8, BLOCK), jnp.bfloat16)
        visible = lax.broadcasted_iota(jnp.int32, (BLOCK, BLOCK), 1) >= lax.broadcasted_iota(jnp.int32, (BLOCK, BLOCK), 0)
        part = lambda i, j: rbuf[turn, i, j * per : (j + 1) * per].reshape(BLOCK, HEAD)
        for j in range(blocks):
            keys = part(1, j)
            values = jnp.concatenate([part(2, j).T, ones], axis=0)
            scores = [_dot(keys, part(0, i), 1, 1) for i in range(j, blocks)]
            weights, keeps = [], []
            for i, s in zip(range(j, blocks), scores):
                if i == j:
                    s = jnp.where(visible, s, 2 * NEG)
                top = s.max(axis=0, keepdims=True)
                if j:
                    old = top_s[i : i + 1, :]
                    top = jnp.maximum(old, top)
                    keeps.append(jnp.exp2((old - top) * e))
                else:
                    keeps.append(None)
                top_s[i : i + 1, :] = top
                weights.append(jnp.exp2((s - top) * e).astype(jnp.bfloat16))
            for i, p, keep in zip(range(j, blocks), weights, keeps):
                new = _dot(values, p, 1, 0)
                if j:
                    new = mix_s[i - 1] * keep + new
                if i == j:
                    done = (new[:HEAD] * (1 / new[HEAD : HEAD + 1])).T.astype(jnp.bfloat16)
                    obuf[i * per : (i + 1) * per] = done.reshape(per, PAIR, HEAD)
                else:
                    mix_s[i - 1] = new

    def outs(turn):
        for n, p in enumerate(peers):
            yield remote(obuf.at[p], seen.at[turn, chip], o_send.at[n], o_recv.at[turn, chip], 2 * p + core)

    def halves(n):
        return remote(yacc.at[n, other, :], ypeer.at[n], y_send.at[n], y_recv.at[n], partner)

    def stages(stage, _):
        first = UNITS * jnp.minimum(stage, STEPS) + CUTS * jnp.maximum(stage - LAG, 0)

        @pl.when(stage >= LAG)
        def _():
            turn = lax.rem(stage - LAG, TURNS)
            for p in peers:
                remote(obuf.at[p], seen.at[turn, p], o_send.at[0], o_recv.at[turn, p], 2 * p + core).wait_recv()

            def chunk(n, fresh):
                slot = arrive(first + n)
                lhs = jnp.concatenate([seen[turn, h] for h in range(CHIPS)], axis=1)
                for h in range(4):
                    if h < 3:
                        got = _dot(lhs, ring[slot, h * WIDE : (h + 1) * WIDE, :], 1, 0)
                    else:
                        got = _dot(lhs, jnp.concatenate([ring[slot, 3 * WIDE :, :512], ring[slot, 3 * WIDE :, 512:]], axis=0), 1, 0)
                    here = slice(h * WIDE, min((h + 1) * WIDE, CUT))
                    if fresh:
                        yacc[n, :, here] = got
                    else:
                        yacc[n, :, here] += got
                start(first + n + SLOTS)

            @pl.when(stage == LAG)
            def _():
                lax.fori_loop(0, CUTS, lambda n, _: chunk(n, True), None)

            @pl.when(stage > LAG)
            def _():
                def more(n, _):
                    chunk(n, False)

                    @pl.when((stage == STEPS + LAG - 1) & (n > 0))
                    def _():
                        halves(n - 1).start()

                lax.fori_loop(0, CUTS, more, None)

        @pl.when(stage < STEPS)
        def _():
            projections(stage, first + CUTS * jnp.minimum(jnp.maximum(stage - LAG + 1, 0), 1))

        @pl.when((stage >= 1) & (stage <= STEPS))
        def _():
            turn = lax.rem(stage - 1, TURNS)
            for i in range(3):
                for p in peers:
                    remote(sbuf.at[i, p], rbuf.at[turn, i, p], q_send.at[i, 0], q_recv.at[turn, i, p], 2 * p + core).wait_recv()

        @pl.when(stage < STEPS)
        def _():
            ship(2, lax.rem(stage, TURNS))

        @pl.when((stage >= 1) & (stage <= STEPS))
        def _():
            turn = lax.rem(stage - 1, TURNS)

            @pl.when(stage > 1)
            def _():
                for copy in outs(turn):
                    copy.wait_send()

            attend(turn)
            for copy in outs(turn):
                copy.start()
            seen[turn, chip] = obuf[chip]

        @pl.when(stage == STEPS)
        def _():
            for n in range(CUTS):
                swap(n).wait_send()
            for n in range(CUTS):
                from_x(n, pl.ds(0, OWN), x_sem).start()

    lax.fori_loop(0, STEPS + LAG, stages, None)
    halves(CUTS - 1).start()
    for i in range(3):
        for copy in sends(i, 0):
            copy.wait_send()
    for copy in outs(0):
        copy.wait_send()

    def result(n):
        return pltpu.make_async_copy(a_buf.at[n, pl.ds(OWN, OWN), :], y_hbm.at[:, pl.ds(n * CUT, CUT)], out_sem.at[n])

    for n in range(CUTS):
        from_x(n, pl.ds(0, OWN), x_sem).wait()
        halves(n).wait_recv()
        total = yacc[n, mine, :] + ypeer[n]
        a_buf[n, OWN:, :] = (a_buf[n, :OWN, :].astype(jnp.float32) + total).astype(jnp.bfloat16)
        if n:
            result(n - 1).start()
    result(CUTS - 1).start()
    for n in range(CUTS):
        halves(n).wait_send()
        result(n).wait()


def layer(x, gain, cos, sin, wq, wk, wv, wo):
    dma = pltpu.SemaphoreType.DMA
    anywhere, vmem = pl.BlockSpec(memory_space=pl.ANY), pl.BlockSpec(memory_space=pltpu.VMEM)
    return pl.pallas_call(
        _kernel,
        out_shape=jax.ShapeDtypeStruct((OWN, D), jnp.bfloat16),
        in_specs=[anywhere, vmem, vmem, vmem] + [anywhere] * 4,
        out_specs=anywhere,
        scratch_shapes=[
            pltpu.VMEM((CUTS, PAIR, CUT), jnp.bfloat16),
            pltpu.VMEM((SLOTS, CUT, WIDE), jnp.bfloat16),
            pltpu.VMEM((2, PAIR, WIDE), jnp.float32),
            pltpu.VMEM((CUTS, PAIR, CUT), jnp.float32),
            pltpu.VMEM((CUTS, OWN, CUT), jnp.float32),
            pltpu.VMEM((3, CHIPS, PAIR, HEAD), jnp.bfloat16),
            pltpu.VMEM((TURNS, 3, CHIPS, PAIR, HEAD), jnp.bfloat16),
            pltpu.VMEM((CHIPS, PAIR, HEAD), jnp.bfloat16),
            pltpu.VMEM((TURNS, CHIPS, PAIR, HEAD), jnp.bfloat16),
            pltpu.VMEM((TOKENS // BLOCK, BLOCK), jnp.float32),
            pltpu.VMEM((TOKENS // BLOCK - 1, HEAD + 8, BLOCK), jnp.float32),
            dma((SLOTS,)),
            dma((CUTS,)),
            dma((CUTS,)),
            dma((CUTS,)),
            dma((3, CHIPS - 1)),
            dma((TURNS, 3, CHIPS)),
            dma((CHIPS - 1,)),
            dma((TURNS, CHIPS)),
            dma((CUTS,)),
            dma((CUTS,)),
            dma((CUTS,)),
            dma((CUTS,)),
        ],
        compiler_params=pltpu.CompilerParams(collective_id=0, has_side_effects=True, vmem_limit_bytes=67043328),
        cost_estimate=pl.CostEstimate(flops=8 * OWN * D * D, transcendentals=STEPS * TOKENS * TOKENS, bytes_accessed=4 * D * D),
    )(x, gain, cos, sin, wq, wk, wv, wo)


def solution(mesh):
    def step(x, gain, wq, wk, wv, wo):
        place = lax.div(lax.axis_index("sp"), 2) * PAIR + jnp.arange(PAIR)
        half = HEAD // 2
        angle = place.astype(jnp.float32)[:, None] * THETA ** (-jnp.arange(half, dtype=jnp.float32) / half)
        cos, sin = jnp.cos(angle), jnp.sin(angle)
        return layer(x, gain.astype(jnp.float32).reshape(CUTS, 1, CUT), jnp.concatenate([cos, cos], -1), jnp.concatenate([-sin, sin], -1), wq, wk, wv, wo)

    tokens, whole = P(("dp", "sp"), None), P(None, None)
    return jax.shard_map(
        step,
        mesh=mesh,
        in_specs=(tokens, P(None), whole, whole, whole, whole),
        out_specs=tokens,
        check_vma=False,
    )
```

```python
import functools

import jax
import jax.numpy as jnp
from jax import lax
from jax.experimental import pallas as pl
from jax.experimental.pallas import tpu as pltpu
from jax.sharding import PartitionSpec as P

HEAD = 128
THETA = 10000
NEG = -1e30
LOG2E = 1.4426950408889634

D = 14336
OWN = 128
PAIR = 256
CHIPS = 8
STEPS = 7
CUT = 3584
CUTS = D // CUT
WIDE = CHIPS * HEAD
SLOTS = 3
LAG = 3
TURNS = 3
TOKENS = CHIPS * PAIR
BLOCK = 512
UNITS = 3 * CUTS
MIDDLE, LATE = LAG * UNITS, LAG * UNITS + (STEPS - LAG) * (UNITS + CUTS)
TOTAL = STEPS * CUTS * 4


def _dot(a, b, ca, cb):
    return lax.dot_general(a, b, (((ca,), (cb,)), ((), ())), preferred_element_type=jnp.float32)


def _kernel(x_hbm, gain_ref, cos_ref, sin_ref, wq, wk, wv, wo, y_hbm, a_buf, ring, acc, yacc, ypeer, sbuf, rbuf, obuf, seen, top_s, mix_s,
            ring_sem, x_in, a_send, a_recv, q_send, q_recv, o_send, o_recv, y_send, y_recv, x_sem, out_sem):
    me = lax.axis_index("sp")
    core, chip = lax.rem(me, 2), lax.div(me, 2)
    partner = me + 1 - 2 * core
    mine = pl.ds(pl.multiple_of(core * OWN, OWN), OWN)
    other = pl.ds(pl.multiple_of((1 - core) * OWN, OWN), OWN)
    peers = [lax.rem(chip + n, CHIPS) for n in range(1, CHIPS)]

    def remote(src, dst, send, recv, device):
        return pltpu.make_async_remote_copy(src_ref=src, dst_ref=dst, send_sem=send, recv_sem=recv, device_id={"sp": device},
                                            device_id_type=pl.DeviceIdType.MESH)

    def start(t):
        early, late = t < MIDDLE, t >= LATE
        stage = jnp.where(early, lax.div(t, UNITS),
                          jnp.where(late, STEPS + lax.div(t - LATE, CUTS), LAG + lax.div(t - MIDDLE, UNITS + CUTS)))
        unit = jnp.where(early, CUTS + lax.rem(t, UNITS),
                         jnp.where(late, lax.rem(t - LATE, CUTS), lax.rem(t - MIDDLE, UNITS + CUTS)))
        slot = lax.rem(t, SLOTS)

        def fetch(w, row, column, rows, columns, to_row, to_column):
            part = w.at[pl.ds(pl.multiple_of(row, 128), rows), pl.ds(pl.multiple_of(column, 128), columns)]
            to = ring.at[slot, pl.ds(to_row, rows), pl.ds(to_column, columns)]
            pltpu.make_async_copy(part, to, ring_sem.at[slot]).start()

        for i, w in enumerate((wq, wk, wv)):

            @pl.when((unit >= CUTS * (i + 1)) & (unit < CUTS * (i + 2)) & (t < TOTAL))
            def _():
                for h in range(2):
                    fetch(w, (unit - CUTS * (i + 1)) * CUT + h * (CUT // 2), (core * STEPS + stage) * WIDE, CUT // 2, WIDE, h * (CUT // 2), 0)

        @pl.when((unit < CUTS) & (t < TOTAL))
        def _():
            row, column = (core * STEPS + stage - LAG) * WIDE, unit * CUT
            for h in range(3):
                fetch(wo, row, column + h * WIDE, WIDE, WIDE, h * WIDE, 0)
            for h in range(2):
                fetch(wo, row + h * 512, column + 3 * WIDE, 512, 512, 3 * WIDE, h * 512)

    def arrive(t):
        slot = lax.rem(t, SLOTS)
        pltpu.make_async_copy(wq.at[pl.ds(0, CUT), pl.ds(0, WIDE)], ring.at[slot], ring_sem.at[slot]).wait()
        return slot

    def from_x(n, rows, sem):
        return pltpu.make_async_copy(x_hbm.at[:, pl.ds(n * CUT, CUT)], a_buf.at[n, rows, :], sem.at[n])

    barrier = pltpu.get_barrier_semaphore()
    pl.semaphore_signal(barrier, inc=1, device_id={"sp": partner}, device_id_type=pl.DeviceIdType.MESH)
    for p in peers:
        pl.semaphore_signal(barrier, inc=1, device_id={"sp": 2 * p + core}, device_id_type=pl.DeviceIdType.MESH)
    for n in range(CUTS):
        from_x(n, mine, x_in).start()
    for t in range(SLOTS):
        start(jnp.int32(t))

    def swap(n):
        return remote(a_buf.at[n, mine, :], a_buf.at[n, mine, :], a_send.at[n], a_recv.at[n], partner)

    def swapped(n):
        return remote(a_buf.at[n, other, :], a_buf.at[n, other, :], a_send.at[n], a_recv.at[n], partner)

    for n in range(CUTS):
        from_x(n, mine, x_in).wait()

    def norm(g, _):
        rows = pl.ds(pl.multiple_of(core * OWN + g * 16, 16), 16)
        wide = [a_buf[n, rows, :].astype(jnp.float32) for n in range(CUTS)]
        squares = sum(jnp.sum(w * w, axis=1, keepdims=True) for w in wide)
        scale = lax.rsqrt(squares / D + 1e-6)
        for n in range(CUTS):
            a_buf[n, rows, :] = (a_buf[n, rows, :].astype(jnp.float32) * scale * gain_ref[:, n * CUT : (n + 1) * CUT]).astype(jnp.bfloat16)

    lax.fori_loop(0, OWN // 16, norm, None)
    pl.semaphore_wait(barrier, CHIPS)
    for n in range(CUTS):
        swap(n).start()
    swapped(0).wait_recv()

    def sends(i, turn):
        for n, p in enumerate(peers):
            yield remote(sbuf.at[i, p], rbuf.at[turn, i, chip], q_send.at[i, n], q_recv.at[turn, i, chip], 2 * p + core)

    def ship(i, turn):
        for copy in sends(i, turn):
            copy.start()
        rbuf[turn, i, chip] = sbuf[i, chip]

    def piece(turn, j, between=lambda h: None):
        e = HEAD**-0.5 * LOG2E
        blocks = TOKENS // BLOCK
        per = BLOCK // PAIR
        part = lambda i, j: rbuf[turn, i, j * per : (j + 1) * per].reshape(BLOCK, HEAD)
        keys = part(1, j)
        values = jnp.concatenate([part(2, j).T, jnp.ones((8, BLOCK), jnp.bfloat16)], axis=0)
        strips = list(range(j, blocks))
        for h, some in enumerate((strips[: (blocks - j + 1) // 2], strips[(blocks - j + 1) // 2 :])):
            scores = [_dot(keys, part(0, i), 1, 1) for i in some]
            between(h)
            weights, keeps = [], []
            for i, s in zip(some, scores):
                if i == j:
                    visible = lax.broadcasted_iota(jnp.int32, (BLOCK, BLOCK), 1) >= lax.broadcasted_iota(jnp.int32, (BLOCK, BLOCK), 0)
                    s = jnp.where(visible, s, 2 * NEG)
                top = s.max(axis=0, keepdims=True)
                keep = None
                if j:
                    old = top_s[i : i + 1, :]
                    top = jnp.maximum(old, top)
                    keep = jnp.exp2((old - top) * e)
                top_s[i : i + 1, :] = top
                weights.append(jnp.exp2((s - top) * e).astype(jnp.bfloat16))
                keeps.append(keep)
            for i, p, keep in zip(some, weights, keeps):
                new = _dot(values, p, 1, 0)
                if j:
                    new = mix_s[i - 1] * keep + new
                if i == j:
                    done = (new[:HEAD] * (1 / new[HEAD : HEAD + 1])).T.astype(jnp.bfloat16)
                    obuf[i * per : (i + 1) * per] = done.reshape(per, PAIR, HEAD)
                else:
                    mix_s[i - 1] = new

    def outs(turn):
        for n, p in enumerate(peers):
            yield remote(obuf.at[p], seen.at[turn, chip], o_send.at[n], o_recv.at[turn, chip], 2 * p + core)

    def gathered(stage):
        turn = lax.rem(stage - 1, TURNS)
        for i in range(3):
            for p in peers:
                remote(sbuf.at[i, p], rbuf.at[turn, i, p], q_send.at[i, 0], q_recv.at[turn, i, p], 2 * p + core).wait_recv()

        @pl.when(stage > 1)
        def _():
            for copy in outs(turn):
                copy.wait_send()

    def projections(stage, first):
        turn = lax.rem(stage, TURNS)

        def free(i):
            @pl.when(stage > 0)
            def _():
                for copy in sends(i, turn):
                    copy.wait_send()

        def settle(i):
            free(i)
            for h in range(CHIPS):
                sbuf[i, h] = acc[:, h * HEAD : (h + 1) * HEAD].astype(jnp.bfloat16)

        def turn_in_place(i):
            for h in range(CHIPS):
                t = sbuf[i, h].astype(jnp.float32)
                sbuf[i, h] = (t * cos_ref[...] + pltpu.roll(t, HEAD // 2, 1) * sin_ref[...]).astype(jnp.bfloat16)

        for i in range(3):

            def chunk(n, fresh):
                t = first + CUTS * i + n
                slot = arrive(t)
                if fresh and i:
                    turn_in_place(i - 1)
                got = _dot(a_buf[n], ring[slot], 1, 0)
                if fresh:
                    acc[...] = got
                else:
                    acc[...] += got
                start(t + SLOTS)

            if i:
                settle(i - 1)
            if i == 2:

                @pl.when(stage > 0)
                def _():
                    gathered(stage)
                    for n in range(CUTS):
                        t = first + CUTS * i + n
                        slot = arrive(t)
                        if n == 0:
                            turn_in_place(i - 1)

                        def half(h):
                            here = slice(h * (WIDE // 2), (h + 1) * (WIDE // 2))
                            got = _dot(a_buf[n], ring[slot, :, here], 1, 0)
                            if n:
                                acc[:, here] += got
                            else:
                                acc[:, here] = got

                        piece(lax.rem(stage - 1, TURNS), n, half)
                        start(t + SLOTS)

                @pl.when(stage == 0)
                def _():
                    chunk(0, True)
                    lax.fori_loop(1, CUTS, lambda n, _: chunk(n, False), None)

                ship(i - 1, turn)
                continue
            chunk(0, True)

            def more(n, _):
                if i == 0:

                    @pl.when(stage == 0)
                    def _():
                        swapped(n).wait_recv()

                chunk(n, False)

            lax.fori_loop(1, CUTS, more, None)
            if i:
                ship(i - 1, turn)
        settle(2)

    def halves(n):
        return remote(yacc.at[n, other, :], ypeer.at[n], y_send.at[n], y_recv.at[n], partner)

    def stages(stage, _):
        first = UNITS * jnp.minimum(stage, STEPS) + CUTS * jnp.maximum(stage - LAG, 0)

        @pl.when(stage >= LAG)
        def _():
            turn = lax.rem(stage - LAG, TURNS)
            for p in peers:
                remote(obuf.at[p], seen.at[turn, p], o_send.at[0], o_recv.at[turn, p], 2 * p + core).wait_recv()

            def chunk(n, fresh):
                slot = arrive(first + n)
                lhs = jnp.concatenate([seen[turn, h] for h in range(CHIPS)], axis=1)
                for h in range(4):
                    if h < 3:
                        got = _dot(lhs, ring[slot, h * WIDE : (h + 1) * WIDE, :], 1, 0)
                    else:
                        got = _dot(lhs, jnp.concatenate([ring[slot, 3 * WIDE :, :512], ring[slot, 3 * WIDE :, 512:]], axis=0), 1, 0)
                    here = slice(h * WIDE, min((h + 1) * WIDE, CUT))
                    if fresh:
                        yacc[n, :, here] = got
                    else:
                        yacc[n, :, here] += got
                start(first + n + SLOTS)

            @pl.when(stage == LAG)
            def _():
                lax.fori_loop(0, CUTS, lambda n, _: chunk(n, True), None)

            @pl.when(stage > LAG)
            def _():
                def more(n, _):
                    chunk(n, False)

                    @pl.when((stage == STEPS + LAG - 1) & (n > 0))
                    def _():
                        halves(n - 1).start()

                lax.fori_loop(0, CUTS, more, None)

        @pl.when(stage < STEPS)
        def _():
            projections(stage, first + CUTS * jnp.minimum(jnp.maximum(stage - LAG + 1, 0), 1))

        @pl.when(stage == STEPS)
        def _():
            gathered(stage)
            for j in range(TOKENS // BLOCK):
                piece(lax.rem(stage - 1, TURNS), j)

        @pl.when((stage >= 1) & (stage <= STEPS))
        def _():
            turn = lax.rem(stage - 1, TURNS)
            for copy in outs(turn):
                copy.start()
            seen[turn, chip] = obuf[chip]

        @pl.when(stage < STEPS)
        def _():
            ship(2, lax.rem(stage, TURNS))

        @pl.when(stage == STEPS)
        def _():
            for n in range(CUTS):
                swap(n).wait_send()
            for n in range(CUTS):
                from_x(n, pl.ds(0, OWN), x_sem).start()

    lax.fori_loop(0, STEPS + LAG, stages, None)
    halves(CUTS - 1).start()
    for i in range(3):
        for copy in sends(i, 0):
            copy.wait_send()
    for copy in outs(0):
        copy.wait_send()

    def result(n):
        return pltpu.make_async_copy(a_buf.at[n, pl.ds(OWN, OWN), :], y_hbm.at[:, pl.ds(n * CUT, CUT)], out_sem.at[n])

    for n in range(CUTS):
        from_x(n, pl.ds(0, OWN), x_sem).wait()
        halves(n).wait_recv()
        total = yacc[n, mine, :] + ypeer[n]
        a_buf[n, OWN:, :] = (a_buf[n, :OWN, :].astype(jnp.float32) + total).astype(jnp.bfloat16)
        if n:
            result(n - 1).start()
    result(CUTS - 1).start()
    for n in range(CUTS):
        halves(n).wait_send()
        result(n).wait()


def layer(x, gain, cos, sin, wq, wk, wv, wo):
    dma = pltpu.SemaphoreType.DMA
    anywhere, vmem = pl.BlockSpec(memory_space=pl.ANY), pl.BlockSpec(memory_space=pltpu.VMEM)
    return pl.pallas_call(
        _kernel,
        out_shape=jax.ShapeDtypeStruct((OWN, D), jnp.bfloat16),
        in_specs=[anywhere, vmem, vmem, vmem] + [anywhere] * 4,
        out_specs=anywhere,
        scratch_shapes=[
            pltpu.VMEM((CUTS, PAIR, CUT), jnp.bfloat16),
            pltpu.VMEM((SLOTS, CUT, WIDE), jnp.bfloat16),
            pltpu.VMEM((PAIR, WIDE), jnp.float32),
            pltpu.VMEM((CUTS, PAIR, CUT), jnp.float32),
            pltpu.VMEM((CUTS, OWN, CUT), jnp.float32),
            pltpu.VMEM((3, CHIPS, PAIR, HEAD), jnp.bfloat16),
            pltpu.VMEM((TURNS, 3, CHIPS, PAIR, HEAD), jnp.bfloat16),
            pltpu.VMEM((CHIPS, PAIR, HEAD), jnp.bfloat16),
            pltpu.VMEM((TURNS, CHIPS, PAIR, HEAD), jnp.bfloat16),
            pltpu.VMEM((TOKENS // BLOCK, BLOCK), jnp.float32),
            pltpu.VMEM((TOKENS // BLOCK - 1, HEAD + 8, BLOCK), jnp.float32),
            dma((SLOTS,)),
            dma((CUTS,)),
            dma((CUTS,)),
            dma((CUTS,)),
            dma((3, CHIPS - 1)),
            dma((TURNS, 3, CHIPS)),
            dma((CHIPS - 1,)),
            dma((TURNS, CHIPS)),
            dma((CUTS,)),
            dma((CUTS,)),
            dma((CUTS,)),
            dma((CUTS,)),
        ],
        compiler_params=pltpu.CompilerParams(collective_id=0, has_side_effects=True, vmem_limit_bytes=67043328),
        cost_estimate=pl.CostEstimate(flops=8 * OWN * D * D, transcendentals=STEPS * TOKENS * TOKENS, bytes_accessed=4 * D * D),
    )(x, gain, cos, sin, wq, wk, wv, wo)


def solution(mesh):
    def step(x, gain, wq, wk, wv, wo):
        place = lax.div(lax.axis_index("sp"), 2) * PAIR + jnp.arange(PAIR)
        half = HEAD // 2
        angle = place.astype(jnp.float32)[:, None] * THETA ** (-jnp.arange(half, dtype=jnp.float32) / half)
        cos, sin = jnp.cos(angle), jnp.sin(angle)
        return layer(x, gain.astype(jnp.float32).reshape(1, D), jnp.concatenate([cos, cos], -1), jnp.concatenate([-sin, sin], -1), wq, wk, wv, wo)

    tokens, whole = P(("dp", "sp"), None), P(None, None)
    return jax.shard_map(
        step,
        mesh=mesh,
        in_specs=(tokens, P(None), whole, whole, whole, whole),
        out_specs=tokens,
        check_vma=False,
    )
```
